512 devices in a mesh: grp: 16 (over z, core), cp: 32 (over y, x).
Axes of the slice: x: 4, y: 8, z: 8, core: 2. Of those that a mesh axis runs over, the one named last changes fastest.
Arguments:
- query: bfloat16 [131072, 2048], P(('grp', 'cp')), may hold values from -6 to 6
- key: bfloat16 [131072, 512], P(('grp', 'cp')), may hold values from -6 to 6
- value: bfloat16 [131072, 512], P(('grp', 'cp')), may hold values from -6 to 6
- output_gradient: bfloat16 [131072, 2048], P(('grp', 'cp')), may hold values from -0.59765625 to 0.59765625
- lse: bfloat16 [131072, 16], P(('grp', 'cp')), may hold values from 1 to 3
- delta: bfloat16 [131072, 16], P(('grp', 'cp')), may hold values from -6 to 6
- lengths: int32 [32], replicated, may hold values from 1 to 8192, as said below
- plan: int32 [8192], P(('grp', 'cp')), may hold values from -1 to 30, as said below
Outputs:
- dquery: bfloat16 [131072, 2048], P(('grp', 'cp'))
- dkey: bfloat16 [131072, 512], P(('grp', 'cp'))
- dvalue: bfloat16 [131072, 512], P(('grp', 'cp'))
The draws below stay inside these ranges and needn't reach their ends.
Inputs may be any that keep to these rules, and one draw needn't show every extreme that they name: `lengths`: in order; they sum to 131072, and the longest is 8192. `plan`: a block's entry is -1 or a member index of its own group below the member that holds the block, whose shard holds tokens of the document of the block's first row; the blocks of one device name distinct members.
All inputs are finite; a program needn't handle non-finite values.
Results may differ from the reference program's by a relative error of at most 0.0061.
Values may be sent and summed in bfloat16 or wider, within the bound.
No kernel may reach another device: no remote copies, remote signals or barrier semaphores. Data moves between devices by JAX's collectives and lax.ppermute only.
A program may use at most 128 MiB of HBM per device.

```python
import jax
import jax.numpy as jnp
from jax import lax

QUERY_HEADS = 16
KEY_VALUE_HEADS = 4
HEAD_SIZE = 128
QB = 16
TOK_DEV = 256
ROUTED_BLOCKS = 16
PACKED_TOKENS = 131072
NBLOCKS = 8192
NDOCS = 32
MOST_DOC = 8192
N_CP = 32
DEVICES = 512


def shared_lengths(key):
    base_key = jax.random.fold_in(key, 7717)
    count = NDOCS - 1
    rest = PACKED_TOKENS - MOST_DOC
    share = rest // count
    extra = rest - share * count
    others = (share + (jnp.arange(count, dtype=jnp.int32) < extra).astype(jnp.int32)).astype(jnp.int32)

    def mover(turn, current):
        turn_key = jax.random.fold_in(base_key, turn + 11)
        pair = jax.random.randint(jax.random.fold_in(turn_key, 1), (2,), 0, count, dtype=jnp.int32)
        first = pair[0]
        second = pair[1]
        room = jnp.minimum(MOST_DOC - current[first], current[second] - 1)
        amount = jax.random.randint(jax.random.fold_in(turn_key, 2), (), 0, room + 1, dtype=jnp.int32)
        return current.at[first].add(amount).at[second].add(-amount)
    others = lax.fori_loop(0, 4 * count, mover, others)
    full = jnp.concatenate([jnp.full((1,), MOST_DOC, jnp.int32), others])
    return jax.random.permutation(jax.random.fold_in(base_key, 3), full).astype(jnp.int32)


def draw_lengths(key, part):
    return shared_lengths(key)


def draw_plan(key, part):
    lengths = shared_lengths(key)
    ends = jnp.cumsum(lengths).astype(jnp.int32)
    starts = (ends - lengths).astype(jnp.int32)
    block_first = jnp.arange(NBLOCKS, dtype=jnp.int32) * QB
    block_doc = jnp.sum((ends[None, :] <= block_first[:, None]).astype(jnp.int32), axis=1)
    doc_start = starts[block_doc].reshape(DEVICES, ROUTED_BLOCKS)
    devices = jnp.arange(DEVICES, dtype=jnp.int32)
    group_member = devices % N_CP
    group_first = devices - group_member
    peer_devices = jnp.arange(N_CP, dtype=jnp.int32)
    owner_end = (group_first[:, None] + peer_devices[None, :]) * TOK_DEV + TOK_DEV
    eligible = (peer_devices[None, None, :] <= group_member[:, None, None] - 1) & (owner_end[:, None, :] > doc_start[:, :, None])
    extra_scores = jnp.where(peer_devices[None, None, :] == group_member[:, None, None] - 1, (1 << 20) * N_CP, 0).astype(jnp.int32)
    score_matrix = jax.random.randint(jax.random.fold_in(key, 5), (DEVICES, ROUTED_BLOCKS, N_CP), 0, 1 << 20, dtype=jnp.int32) * N_CP + peer_devices[None, None, :] + extra_scores

    def assign(index, carry):
        used, chosen = carry
        open_peer = lax.dynamic_index_in_dim(eligible, index, 1, False) & jnp.logical_not(used)
        marked = jnp.where(open_peer, lax.dynamic_index_in_dim(score_matrix, index, 1, False), -1)
        best = jnp.argmax(marked, axis=1).astype(jnp.int32)
        found = jnp.max(marked, axis=1) >= 0
        owner = jnp.where(found, best, -1).astype(jnp.int32)
        used = used | (peer_devices[None, :] == best[:, None]) & found[:, None]
        chosen = lax.dynamic_update_slice_in_dim(chosen, owner[:, None], index, 1)
        return (used, chosen)
    start = (jnp.zeros((DEVICES, N_CP), bool), jnp.full((DEVICES, ROUTED_BLOCKS), -1, jnp.int32))
    used, chosen = lax.fori_loop(0, ROUTED_BLOCKS, assign, start)
    return chosen.reshape(NBLOCKS).astype(jnp.int32)


def shard_levels(key, shape, cuts, smallest, high):
    def one(dim, shards_of):
        steps = jax.random.uniform(jax.random.fold_in(jax.random.fold_in(key, 6), dim), (shards_of,), jnp.float32, smallest / len(cuts), high / len(cuts))
        return jnp.repeat(jnp.exp(steps), shape[dim] // shards_of).reshape((-1,) + (1,) * (len(shape) - dim - 1))

    loudness = one(*cuts[0])
    for cut in cuts[1:]:
        loudness = loudness * one(*cut)
    return loudness


def bell_draw(stream_key, extent, deviation, limit, shards=(), kind=jnp.bfloat16):
    array = deviation * jax.random.normal(stream_key, extent, jnp.float32)
    if shards:
        array = array * shard_levels(stream_key, extent, shards, -0.22, 0.18)
    return jnp.clip(array, -limit, limit).astype(kind)


def setup_inputs(seed: int = 0) -> dict:
    arg_keys = jax.random.split(jax.random.key(seed), 9)
    return {
        "query": bell_draw(arg_keys[0], (PACKED_TOKENS, QUERY_HEADS * HEAD_SIZE), 1.0, 6.0, ((0, 512),)),
        "key": bell_draw(arg_keys[1], (PACKED_TOKENS, KEY_VALUE_HEADS * HEAD_SIZE), 1.0, 6.0, ((0, 512),)),
        "value": bell_draw(arg_keys[2], (PACKED_TOKENS, KEY_VALUE_HEADS * HEAD_SIZE), 1.0, 6.0, ((0, 512),)),
        "output_gradient": bell_draw(arg_keys[3], (PACKED_TOKENS, QUERY_HEADS * HEAD_SIZE), 0.1, 0.59765625, ((0, 512),)),
        "lse": jnp.clip(1.0 + 2.0 * jax.random.uniform(arg_keys[4], (PACKED_TOKENS, QUERY_HEADS), jnp.float32) ** shard_levels(arg_keys[4], (PACKED_TOKENS, QUERY_HEADS), ((0, 512),), -0.2, 0.2), 1.0, 3.0).astype(jnp.bfloat16),
        "delta": bell_draw(arg_keys[5], (PACKED_TOKENS, QUERY_HEADS), 1.0, 6.0, ((0, 512),)),
        "lengths": draw_lengths(jax.random.fold_in(arg_keys[8], 71), 0),
        "plan": draw_plan(jax.random.fold_in(arg_keys[8], 71), 0),
    }


def doc_ids(position, doc_ends):
    return jnp.sum((doc_ends[None, :] <= position[:, None]).astype(jnp.int32), axis=1).astype(jnp.int32)


def lowered(values):
    return lax.optimization_barrier(values.astype(jnp.bfloat16)).astype(jnp.float32)


def head_grads(queries, grad_rows, lse_rows, delta_rows, keys_head, values_head, allowed):
    factor = HEAD_SIZE ** -0.5
    score_matrix = jnp.einsum("rgd,cd->rgc", queries, keys_head) * factor
    shifted = jnp.where(allowed[:, None, :], score_matrix - lse_rows[:, :, None], -jnp.inf)
    probs = jnp.exp(shifted)
    dprobs = jnp.einsum("rgd,cd->rgc", grad_rows, values_head)
    dscores = probs * (dprobs - delta_rows[:, :, None])
    probs_low = lowered(probs)
    dscores_low = lowered(dscores)
    value_gradient = jnp.einsum("rgc,rgd->cd", probs_low, grad_rows)
    key_gradient = jnp.einsum("rgc,rgd->cd", dscores_low, queries) * factor
    grad_query = jnp.einsum("rgc,cd->rgd", dscores_low, keys_head) * factor
    return grad_query, key_gradient, value_gradient


def attention_grads(query, output_gradient, lse, delta, key, value, allowed):
    query_count = query.shape[0]
    key_count = key.shape[0]
    query_group = QUERY_HEADS // KEY_VALUE_HEADS
    query_per_head = jnp.moveaxis(query.astype(jnp.float32).reshape(query_count, KEY_VALUE_HEADS, query_group, HEAD_SIZE), 1, 0)
    gradient_per_head = jnp.moveaxis(output_gradient.astype(jnp.float32).reshape(query_count, KEY_VALUE_HEADS, query_group, HEAD_SIZE), 1, 0)
    logsumexp_per_head = jnp.moveaxis(lse.astype(jnp.float32).reshape(query_count, KEY_VALUE_HEADS, query_group), 1, 0)
    delta_per_head = jnp.moveaxis(delta.astype(jnp.float32).reshape(query_count, KEY_VALUE_HEADS, query_group), 1, 0)
    key_per_head = jnp.moveaxis(key.astype(jnp.float32).reshape(key_count, KEY_VALUE_HEADS, HEAD_SIZE), 1, 0)
    value_per_head = jnp.moveaxis(value.astype(jnp.float32).reshape(key_count, KEY_VALUE_HEADS, HEAD_SIZE), 1, 0)

    def per_head(pieces):
        return head_grads(pieces[0], pieces[1], pieces[2], pieces[3], pieces[4], pieces[5], allowed)

    grad_query, key_gradient, value_gradient = lax.map(per_head, (query_per_head, gradient_per_head, logsumexp_per_head, delta_per_head, key_per_head, value_per_head))
    return (jnp.moveaxis(grad_query, 0, 1).reshape(query_count, QUERY_HEADS * HEAD_SIZE),
            jnp.moveaxis(key_gradient, 0, 1).reshape(key_count, KEY_VALUE_HEADS * HEAD_SIZE),
            jnp.moveaxis(value_gradient, 0, 1).reshape(key_count, KEY_VALUE_HEADS * HEAD_SIZE))


def reference(query, key, value, output_gradient, lse, delta, lengths, plan):
    shard_count = PACKED_TOKENS // TOK_DEV
    block_count = TOK_DEV // QB
    key_value_width = KEY_VALUE_HEADS * HEAD_SIZE
    width_q = QUERY_HEADS * HEAD_SIZE
    doc_ends = jnp.cumsum(lengths).astype(jnp.int32)
    pad_rows = jnp.zeros((TOK_DEV, key_value_width), key.dtype)
    key_pad = jnp.concatenate([pad_rows, key], axis=0)
    value_pad = jnp.concatenate([pad_rows, value], axis=0)
    key_shards = key.reshape(shard_count, TOK_DEV, key_value_width)
    value_shards = value.reshape(shard_count, TOK_DEV, key_value_width)
    offsets = jnp.arange(TOK_DEV, dtype=jnp.int32)

    def step(carry, shard_id):
        dk_acc, dv_acc = carry
        first_row = shard_id * TOK_DEV
        rows_query = lax.dynamic_slice_in_dim(query, first_row, TOK_DEV, 0)
        rows_grad = lax.dynamic_slice_in_dim(output_gradient, first_row, TOK_DEV, 0)
        rows_lse = lax.dynamic_slice_in_dim(lse, first_row, TOK_DEV, 0)
        rows_delta = lax.dynamic_slice_in_dim(delta, first_row, TOK_DEV, 0)
        position = first_row + offsets
        own_doc = doc_ids(position, doc_ends)
        owners = lax.dynamic_slice_in_dim(plan, shard_id * block_count, block_count, 0)
        member_id = (shard_id % N_CP).astype(jnp.int32)
        owners_row = jnp.repeat(owners, QB)
        skip_prev = (owners_row == member_id - 1) & (member_id >= 1)
        key_rows = lax.dynamic_slice_in_dim(key_pad, first_row, 2 * TOK_DEV, 0)
        value_rows = lax.dynamic_slice_in_dim(value_pad, first_row, 2 * TOK_DEV, 0)
        key_pos = first_row - TOK_DEV + jnp.arange(2 * TOK_DEV, dtype=jnp.int32)
        key_doc = doc_ids(key_pos, doc_ends)
        allowed = (own_doc[:, None] == key_doc[None, :]) & (key_pos[None, :] <= position[:, None]) & (key_pos[None, :] >= 0)
        allowed = allowed & jnp.logical_not(skip_prev[:, None] & (key_pos[None, :] < first_row))
        dq_local, dk_local, dv_local = attention_grads(rows_query, rows_grad, rows_lse, rows_delta, key_rows, value_rows, allowed)
        dk_acc = lax.dynamic_update_slice_in_dim(dk_acc, lax.dynamic_slice_in_dim(dk_acc, shard_id, 2, 0) + dk_local.reshape(2, TOK_DEV, key_value_width), shard_id, 0)
        dv_acc = lax.dynamic_update_slice_in_dim(dv_acc, lax.dynamic_slice_in_dim(dv_acc, shard_id, 2, 0) + dv_local.reshape(2, TOK_DEV, key_value_width), shard_id, 0)
        group_first = (shard_id // N_CP) * N_CP
        owner_shard = (group_first + jnp.maximum(owners, 0)).astype(jnp.int32)
        live_block = owners >= 0
        block_key = key_shards[owner_shard]
        block_value = value_shards[owner_shard]
        block_key_pos = owner_shard[:, None] * TOK_DEV + offsets[None, :]
        block_pos = position.reshape(block_count, QB)

        def one_block(b_query, b_grad, b_lse, b_delta, b_key, b_value, b_pos, b_key_pos, b_live):
            allowed_block = b_live & (doc_ids(b_pos, doc_ends)[:, None] == doc_ids(b_key_pos, doc_ends)[None, :]) & (b_key_pos[None, :] <= b_pos[:, None])
            return attention_grads(b_query, b_grad, b_lse, b_delta, b_key, b_value, allowed_block)

        dq_block, dk_block, dv_block = jax.vmap(one_block)(
            rows_query.reshape(block_count, QB, width_q), rows_grad.reshape(block_count, QB, width_q),
            rows_lse.reshape(block_count, QB, QUERY_HEADS), rows_delta.reshape(block_count, QB, QUERY_HEADS),
            block_key, block_value, block_pos, block_key_pos, live_block)
        dk_acc = dk_acc.at[owner_shard + 1].add(dk_block)
        dv_acc = dv_acc.at[owner_shard + 1].add(dv_block)
        grad_query = (dq_local + dq_block.reshape(TOK_DEV, width_q)).astype(jnp.bfloat16)
        return (dk_acc, dv_acc), grad_query

    zeros = jnp.zeros((shard_count + 1, TOK_DEV, key_value_width), jnp.float32)
    (dk_acc, dv_acc), dquery = lax.scan(step, (zeros, zeros), jnp.arange(shard_count, dtype=jnp.int32))
    dkey = dk_acc[1:].reshape(PACKED_TOKENS, key_value_width).astype(jnp.bfloat16)
    dvalue = dv_acc[1:].reshape(PACKED_TOKENS, key_value_width).astype(jnp.bfloat16)
    return dquery.reshape(PACKED_TOKENS, width_q), dkey, dvalue
```

```python
import functools
import math

import jax
import jax.numpy as jnp
from jax import lax
from jax.experimental import pallas as pl
from jax.experimental.pallas import tpu as pltpu
from jax.sharding import Mesh
from jax.sharding import PartitionSpec as P

QUERY_HEADS = 16
KEY_VALUE_HEADS = 4
HEAD_SIZE = 128
GROUP = QUERY_HEADS // KEY_VALUE_HEADS
ROWS = 256
QB = 16
BLOCKS = ROWS // QB
NY = 8
NX = 4
HALVES = 1
HEADS_HALF = KEY_VALUE_HEADS // HALVES
QW = HEADS_HALF * GROUP * HEAD_SIZE
KW = HEADS_HALF * HEAD_SIZE
SLOTS = NY * QB
EXT = 128
LSE_AT = 0
DELTA_AT = 16
LOW_AT = 32
GRP_CP = ("grp", "cp_0", "cp_1")
FACTOR = HEAD_SIZE ** (-0.5)
LOG2E = math.log2(math.e)

F32 = jnp.float32
BF16 = jnp.bfloat16


def dot_nt(a, b):
    return lax.dot_general(a, b, (((1,), (1,)), ((), ())), preferred_element_type=F32)


def dot_nn(a, b):
    return lax.dot_general(a, b, (((1,), (0,)), ((), ())), preferred_element_type=F32)


def dot_tn(a, b):
    return lax.dot_general(a, b, (((0,), (0,)), ((), ())), preferred_element_type=F32)


def tile_grads(keys, values, queries, grads, lse2, delta, mask):
    scores = dot_nt(keys, queries)
    probs = jnp.where(mask, jnp.exp2(scores * (FACTOR * LOG2E) - lse2), 0.0)
    dprobs = dot_nt(values, grads)
    dscores = probs * (dprobs - delta)
    probs_low = probs.astype(BF16)
    dscores_low = dscores.astype(BF16)
    return (
        dot_tn(dscores_low, keys),
        dot_nn(dscores_low, queries),
        dot_nn(probs_low, grads),
    )


def pack_kernel(with_ext, inv_ref, q_ref, g_ref, ext_ref, *out_refs):
    lane = lax.broadcasted_iota(jnp.int32, (QB, EXT), 1)

    def one(yy, carry):
        to = pl.ds(pl.multiple_of(yy * QB, QB), QB)
        for s in range(NX):
            found = inv_ref[s * NY + yy]
            rows = pl.ds(pl.multiple_of(jnp.maximum(found, 0) * QB, QB), QB)
            out_refs[s][to, 0:QW] = q_ref[rows, :]
            out_refs[s][to, QW : 2 * QW] = g_ref[rows, :]
            if with_ext:
                ext = ext_ref[rows, :].astype(F32)
                low = jnp.where(found >= 0, ext, float(ROWS))
                ext = jnp.where(lane >= LOW_AT, low, ext)
                out_refs[s][to, 2 * QW :] = ext.astype(BF16)
        return carry

    lax.fori_loop(0, NY, one, 0)


def pack(half, inv, query, grad, ext):
    with_ext = half == 0
    width = 2 * QW + (EXT if with_ext else 0)
    spec = pl.BlockSpec((ROWS, QW), lambda i, half=half: (0, half))
    return pl.pallas_call(
        functools.partial(pack_kernel, with_ext),
        grid=(1,),
        in_specs=[
            pl.BlockSpec(memory_space=pltpu.SMEM),
            spec,
            spec,
            pl.BlockSpec((ROWS, EXT), lambda i: (0, 0)),
        ],
        out_specs=[pl.BlockSpec((SLOTS, width), lambda i: (0, 0))] * NX,
        out_shape=[jax.ShapeDtypeStruct((SLOTS, width), BF16)] * NX,
        cost_estimate=pl.CostEstimate(
            flops=4 * 10**9, bytes_accessed=6 << 20, transcendentals=0
        ),
        name=f"pack_{half}",
    )(inv, query, grad, ext)


def local_kernel(
    q_ref, g_ref, k_ref, v_ref, pk_ref, pv_ref, ext_ref, low_ref,
    dq_ref, dk_ref, dv_ref, dpk_ref, dpv_ref, stat_ref, acc_ref,
):
    g = pl.program_id(0)

    @pl.when(g == 0)
    def _():
        stat_ref[...] = ext_ref[...].astype(F32).T

    key = lax.broadcasted_iota(jnp.int32, (ROWS, ROWS), 0)
    row = lax.broadcasted_iota(jnp.int32, (ROWS, ROWS), 1)
    low = low_ref[0:1, :]
    mask_prev = key >= low
    mask_own = (key + ROWS >= low) & (key <= row)
    for h in range(GROUP):
        cols = slice(h * HEAD_SIZE, (h + 1) * HEAD_SIZE)
        queries = q_ref[:, cols]
        grads = g_ref[:, cols]
        head = g * GROUP + h
        lse2 = stat_ref[pl.ds(LSE_AT + head, 1), :] * LOG2E
        delta = stat_ref[pl.ds(DELTA_AT + head, 1), :]
        dq0, dk0, dv0 = tile_grads(
            pk_ref[...], pv_ref[...], queries, grads, lse2, delta, mask_prev
        )
        dq1, dk1, dv1 = tile_grads(
            k_ref[...], v_ref[...], queries, grads, lse2, delta, mask_own
        )
        dq_ref[:, cols] = (dq0 + dq1) * FACTOR
        for n, part in enumerate((dk0, dv0, dk1, dv1)):
            if h == 0:
                acc_ref[n] = part
            else:
                acc_ref[n] += part
    dpk_ref[...] = (acc_ref[0] * FACTOR).astype(BF16)
    dpv_ref[...] = acc_ref[1].astype(BF16)
    dk_ref[...] = acc_ref[2] * FACTOR
    dv_ref[...] = acc_ref[3]


def local_grads(query, grad, key, value, prev_key, prev_value, ext, low):
    wide = pl.BlockSpec((ROWS, GROUP * HEAD_SIZE), lambda g: (0, g))
    narrow = pl.BlockSpec((ROWS, HEAD_SIZE), lambda g: (0, g))
    kv = (ROWS, KEY_VALUE_HEADS * HEAD_SIZE)
    return pl.pallas_call(
        local_kernel,
        grid=(KEY_VALUE_HEADS,),
        in_specs=[
            wide, wide, narrow, narrow, narrow, narrow,
            pl.BlockSpec((ROWS, EXT), lambda g: (0, 0)),
            pl.BlockSpec((8, ROWS), lambda g: (0, 0)),
        ],
        out_specs=[wide, narrow, narrow, narrow, narrow],
        out_shape=[
            jax.ShapeDtypeStruct((ROWS, QUERY_HEADS * HEAD_SIZE), F32),
            jax.ShapeDtypeStruct(kv, F32),
            jax.ShapeDtypeStruct(kv, F32),
            jax.ShapeDtypeStruct(kv, BF16),
            jax.ShapeDtypeStruct(kv, BF16),
        ],
        scratch_shapes=[
            pltpu.VMEM((EXT, ROWS), F32),
            pltpu.VMEM((4, ROWS, HEAD_SIZE), F32),
        ],
        cost_estimate=pl.CostEstimate(
            flops=16 * 10**9, bytes_accessed=8 << 20, transcendentals=0
        ),
        name="local_grads",
    )(query, grad, key, value, prev_key, prev_value, ext, low)


def routed_kernel(half, y_ref, kv_ref, *refs):
    slot_refs, ext_refs, refs = refs[:NX], refs[NX : 2 * NX], refs[2 * NX :]
    dq_refs, dkv_ref = refs[:NX], refs[NX]
    yy = pl.program_id(0)

    @pl.when(yy > y_ref[0])
    def _():
        dkv_ref[...] = jnp.zeros_like(dkv_ref)
        for s in range(NX):
            dq_refs[s][...] = jnp.zeros_like(dq_refs[s])

    @pl.when(yy <= y_ref[0])
    def _():
        ext = jnp.concatenate([r[...].astype(F32) for r in ext_refs], axis=0)
        key = lax.broadcasted_iota(jnp.int32, (ROWS, ROWS), 0).astype(F32)
        for g in range(HEADS_HALF):
            heads = [g * GROUP + h for h in range(GROUP)]
            first = half * HEADS_HALF * GROUP
            stat = jnp.concatenate(
                [pltpu.roll(ext, (EXT - first - j) % EXT, 1) for j in heads], axis=0
            ).T
            lse2 = stat[LSE_AT : LSE_AT + 1, :] * LOG2E
            delta = stat[DELTA_AT : DELTA_AT + 1, :]
            mask = key >= stat[LOW_AT : LOW_AT + 1, :]

            def rows_of(base):
                return jnp.concatenate(
                    [
                        r[:, base + j * HEAD_SIZE : base + (j + 1) * HEAD_SIZE]
                        for j in heads
                        for r in slot_refs
                    ],
                    axis=0,
                )

            queries = rows_of(0)
            grads = rows_of(QW)
            keys = kv_ref[:, g * HEAD_SIZE : (g + 1) * HEAD_SIZE]
            values = kv_ref[:, KW + g * HEAD_SIZE : KW + (g + 1) * HEAD_SIZE]
            dq, dk, dv = tile_grads(keys, values, queries, grads, lse2, delta, mask)
            dkv_ref[:, g * HEAD_SIZE : (g + 1) * HEAD_SIZE] = (dk * FACTOR).astype(BF16)
            dkv_ref[:, KW + g * HEAD_SIZE : KW + (g + 1) * HEAD_SIZE] = dv.astype(BF16)
            dq_low = (dq * FACTOR).astype(BF16)
            for n, j in enumerate(heads):
                for s in range(NX):
                    at = (n * NX + s) * QB
                    dq_refs[s][:, j * HEAD_SIZE : (j + 1) * HEAD_SIZE] = dq_low[at : at + QB]


def routed_grads(half, y, kv_all, slots, ext_slots):
    ext_at = 2 * QW // EXT
    return pl.pallas_call(
        functools.partial(routed_kernel, half),
        grid=(NY,),
        in_specs=[
            pl.BlockSpec(memory_space=pltpu.SMEM),
            pl.BlockSpec((ROWS, 2 * KW), lambda i: (i, 0)),
        ]
        + [pl.BlockSpec((QB, 2 * QW), lambda i: (i, 0))] * NX
        + [pl.BlockSpec((QB, EXT), lambda i: (i, ext_at))] * NX,
        out_specs=[pl.BlockSpec((QB, QW), lambda i: (i, 0))] * NX
        + [pl.BlockSpec((ROWS, 2 * KW), lambda i: (i, 0))],
        out_shape=[jax.ShapeDtypeStruct((SLOTS, QW), BF16)] * NX
        + [jax.ShapeDtypeStruct((NY * ROWS, 2 * KW), BF16)],
        cost_estimate=pl.CostEstimate(
            flops=8 * 10**9, bytes_accessed=8 << 20, transcendentals=0
        ),
        name=f"routed_grads_{half}",
    )(y, kv_all, *slots, *ext_slots)


def join_kernel(inv_ref, dq_ref, *refs):
    out_ref = refs[-1]
    out_ref[...] = dq_ref[...].astype(BF16)

    def one(yy, carry):
        at = pl.ds(pl.multiple_of(yy * QB, QB), QB)
        for s in range(NX):
            found = inv_ref[s * NY + yy]

            @pl.when(found >= 0)
            def _(s=s, found=found):
                rows = pl.ds(pl.multiple_of(found * QB, QB), QB)
                for half in range(HALVES):
                    cols = slice(half * QW, (half + 1) * QW)
                    part = refs[half * NX + s][at, :].astype(F32)
                    out_ref[rows, cols] = (dq_ref[rows, cols] + part).astype(BF16)

        return carry

    lax.fori_loop(0, NY, one, 0)


def join_queries(inv, dq_local, returned):
    vmem = pl.BlockSpec(memory_space=pltpu.VMEM)
    return pl.pallas_call(
        join_kernel,
        in_specs=[pl.BlockSpec(memory_space=pltpu.SMEM), vmem] + [vmem] * (NX * HALVES),
        out_specs=vmem,
        out_shape=jax.ShapeDtypeStruct((ROWS, QUERY_HEADS * HEAD_SIZE), BF16),
        cost_estimate=pl.CostEstimate(
            flops=4 * 10**9, bytes_accessed=6 << 20, transcendentals=0
        ),
        name="join_queries",
    )(inv, dq_local, *returned)


def sum_kernel(dk_ref, dv_ref, bk_ref, bv_ref, *refs):
    part_refs, (out_k, out_v) = refs[:HALVES], refs[HALVES:]
    for half in range(HALVES):
        cols = slice(half * KW, (half + 1) * KW)
        part = part_refs[half]
        out_k[:, cols] = (
            dk_ref[:, cols] + bk_ref[:, cols].astype(F32) + part[:, :KW].astype(F32)
        ).astype(BF16)
        out_v[:, cols] = (
            dv_ref[:, cols] + bv_ref[:, cols].astype(F32) + part[:, KW:].astype(F32)
        ).astype(BF16)


def sum_keys(dk, dv, back_k, back_v, parts):
    vmem = pl.BlockSpec(memory_space=pltpu.VMEM)
    shape = jax.ShapeDtypeStruct((ROWS, KEY_VALUE_HEADS * HEAD_SIZE), BF16)
    return pl.pallas_call(
        sum_kernel,
        in_specs=[vmem] * (4 + HALVES),
        out_specs=[vmem, vmem],
        out_shape=[shape, shape],
        name="sum_keys",
    )(dk, dv, back_k, back_v, *parts)


def around(value, steps):
    return lax.ppermute(value, "cp_1", [(i, (i + steps) % NX) for i in range(NX)])


def along(value, steps):
    count = lax.axis_size(GRP_CP)
    first, last = (max(0, -steps), min(count, count - steps))
    return lax.ppermute(value, GRP_CP, [(i, i + steps) for i in range(first, last)])


def on_device(query, key, value, output_gradient, lse, delta, lengths, plan):
    y = lax.axis_index("cp_0")
    x = lax.axis_index("cp_1")
    member = y * NX + x
    shard = lax.axis_index(GRP_CP)
    first_row = shard * ROWS

    kv_halves = [
        jnp.concatenate(
            [key[:, h * KW : (h + 1) * KW], value[:, h * KW : (h + 1) * KW]], axis=1
        )
        for h in range(HALVES)
    ]
    kv_all = [lax.all_gather(kv, "cp_0", axis=0, tiled=True) for kv in kv_halves]
    prev_key = along(key, 1)
    prev_value = along(value, 1)

    order = jnp.arange(lengths.shape[0], dtype=jnp.int32)
    ends = jnp.sum(jnp.where(order[:, None] <= order[None, :], lengths[:, None], 0), axis=0)
    position = first_row + jnp.arange(ROWS, dtype=jnp.int32)
    doc_start = jnp.max(jnp.where(ends[:, None] <= position[None, :], ends[:, None], 0), axis=0)
    row_plan = jnp.repeat(plan, QB)
    skip_prev = (row_plan == member - 1) & (member >= 1)
    low_local = doc_start - (first_row - ROWS)
    low_local = jnp.where(skip_prev, jnp.maximum(low_local, ROWS), low_local)
    low_local = jnp.broadcast_to(low_local[None, :], (8, ROWS))
    target_row = (shard - member + jnp.maximum(row_plan, 0)) * ROWS
    low_routed = jnp.clip(doc_start - target_row, 0, ROWS).astype(BF16)
    ext = jnp.concatenate(
        [
            lse,
            delta,
            jnp.broadcast_to(low_routed[:, None], (ROWS, QUERY_HEADS)),
            jnp.zeros((ROWS, EXT - 3 * QUERY_HEADS), BF16),
        ],
        axis=1,
    )

    steps = jnp.arange(NX, dtype=jnp.int32)
    targets = jnp.arange(NY, dtype=jnp.int32)[None, :] * NX + ((x + steps) % NX)[:, None]
    hits = plan[None, :] == targets.reshape(-1)[:, None]
    inv = jnp.max(jnp.where(hits, jnp.arange(BLOCKS, dtype=jnp.int32)[None, :], -1), axis=1)

    slots = []
    for half in range(HALVES):
        packed = pack(half, inv, query, output_gradient, ext)
        slots.append([packed[0]] + [around(packed[s], s) for s in range(1, NX)])

    dq_local, dk_own, dv_own, dk_prev, dv_prev = local_grads(
        query, output_gradient, key, value, prev_key, prev_value, ext, low_local
    )
    back_k = along(dk_prev, -1)
    back_v = along(dv_prev, -1)
    *kv_all, dq_local = lax.optimization_barrier((*kv_all, dq_local))

    y_table = jnp.reshape(y, (1,)).astype(jnp.int32)
    returned, parts = [], []
    for half in range(HALVES):
        *dq_slots, dkv = routed_grads(half, y_table, kv_all[half], slots[half], slots[0])
        parts.append(lax.psum_scatter(dkv, "cp_0", scatter_dimension=0, tiled=True))
        returned += [dq_slots[0]] + [around(dq_slots[s], -s) for s in range(1, NX)]

    dquery = join_queries(inv, dq_local, returned)
    dkey, dvalue = sum_keys(dk_own, dv_own, back_k, back_v, parts)
    return dquery, dkey, dvalue


def solution(mesh):
    torus = Mesh(mesh.devices.reshape(mesh.shape["grp"], NY, NX), ("grp", "cp_0", "cp_1"))
    split = P(GRP_CP, None)
    return jax.shard_map(
        on_device,
        mesh=torus,
        in_specs=(split,) * 6 + (P(), P(GRP_CP)),
        out_specs=(split,) * 3,
        check_vma=False,
    )
```

```python
import functools
import math

import jax
import jax.numpy as jnp
from jax import lax
from jax.experimental import pallas as pl
from jax.experimental.pallas import tpu as pltpu
from jax.sharding import Mesh
from jax.sharding import PartitionSpec as P

QUERY_HEADS = 16
KEY_VALUE_HEADS = 4
HEAD_SIZE = 128
GROUP = QUERY_HEADS // KEY_VALUE_HEADS
ROWS = 256
QB = 16
BLOCKS = ROWS // QB
NY = 8
NX = 4
HALVES = 1
HEADS_HALF = KEY_VALUE_HEADS // HALVES
QW = HEADS_HALF * GROUP * HEAD_SIZE
KW = HEADS_HALF * HEAD_SIZE
SLOTS = NY * QB
EXT = 128
LSE_AT = 0
DELTA_AT = 16
LOW_AT = 32
GRP_CP = ("grp", "cp_0", "cp_1")
FACTOR = HEAD_SIZE ** (-0.5)
LOG2E = math.log2(math.e)

F32 = jnp.float32
BF16 = jnp.bfloat16


def dot_nt(a, b):
    return lax.dot_general(a, b, (((1,), (1,)), ((), ())), preferred_element_type=F32)


def dot_nn(a, b):
    return lax.dot_general(a, b, (((1,), (0,)), ((), ())), preferred_element_type=F32)


def dot_tn(a, b):
    return lax.dot_general(a, b, (((0,), (0,)), ((), ())), preferred_element_type=F32)


def tile_grads(keys, values, queries, grads, lse2, delta, mask):
    scores = dot_nt(keys, queries)
    probs = jnp.where(mask, jnp.exp2(scores * (FACTOR * LOG2E) - lse2), 0.0)
    dprobs = dot_nt(values, grads)
    dscores = probs * (dprobs - delta)
    probs_low = probs.astype(BF16)
    dscores_low = dscores.astype(BF16)
    return (
        dot_tn(dscores_low, keys),
        dot_nn(dscores_low, queries),
        dot_nn(probs_low, grads),
    )


def pack_kernel(with_ext, inv_ref, q_ref, g_ref, ext_ref, *out_refs):
    lane = lax.broadcasted_iota(jnp.int32, (QB, EXT), 1)

    def one(yy, carry):
        to = pl.ds(pl.multiple_of(yy * QB, QB), QB)
        for s in range(NX):
            found = inv_ref[s * NY + yy]
            rows = pl.ds(pl.multiple_of(jnp.maximum(found, 0) * QB, QB), QB)
            out_refs[s][to, 0:QW] = q_ref[rows, :]
            out_refs[s][to, QW : 2 * QW] = g_ref[rows, :]
            if with_ext:
                ext = ext_ref[rows, :].astype(F32)
                low = jnp.where(found >= 0, ext, float(ROWS))
                ext = jnp.where(lane >= LOW_AT, low, ext)
                out_refs[s][to, 2 * QW :] = ext.astype(BF16)
        return carry

    lax.fori_loop(0, NY, one, 0)


def pack(half, inv, query, grad, ext):
    with_ext = half == 0
    width = 2 * QW + (EXT if with_ext else 0)
    spec = pl.BlockSpec((ROWS, QW), lambda i, half=half: (0, half))
    return pl.pallas_call(
        functools.partial(pack_kernel, with_ext),
        grid=(1,),
        in_specs=[
            pl.BlockSpec(memory_space=pltpu.SMEM),
            spec,
            spec,
            pl.BlockSpec((ROWS, EXT), lambda i: (0, 0)),
        ],
        out_specs=[pl.BlockSpec((SLOTS, width), lambda i: (0, 0))] * NX,
        out_shape=[jax.ShapeDtypeStruct((SLOTS, width), BF16)] * NX,
        cost_estimate=pl.CostEstimate(
            flops=4 * 10**9, bytes_accessed=6 << 20, transcendentals=0
        ),
        name=f"pack_{half}",
    )(inv, query, grad, ext)


def local_kernel(
    q_ref, g_ref, k_ref, v_ref, pk_ref, pv_ref, ext_ref, low_ref,
    dq_ref, dk_ref, dv_ref, prev_ref, stat_ref, acc_ref,
):
    g = pl.program_id(0)

    @pl.when(g == 0)
    def _():
        stat_ref[...] = ext_ref[...].astype(F32).T

    key = lax.broadcasted_iota(jnp.int32, (ROWS, ROWS), 0)
    row = lax.broadcasted_iota(jnp.int32, (ROWS, ROWS), 1)
    low = low_ref[0:1, :]
    mask_prev = key >= low
    mask_own = (key + ROWS >= low) & (key <= row)
    for h in range(GROUP):
        cols = slice(h * HEAD_SIZE, (h + 1) * HEAD_SIZE)
        queries = q_ref[:, cols]
        grads = g_ref[:, cols]
        head = g * GROUP + h
        lse2 = stat_ref[pl.ds(LSE_AT + head, 1), :] * LOG2E
        delta = stat_ref[pl.ds(DELTA_AT + head, 1), :]
        dq0, dk0, dv0 = tile_grads(
            pk_ref[...], pv_ref[...], queries, grads, lse2, delta, mask_prev
        )
        dq1, dk1, dv1 = tile_grads(
            k_ref[...], v_ref[...], queries, grads, lse2, delta, mask_own
        )
        dq_ref[:, cols] = (dq0 + dq1) * FACTOR
        for n, part in enumerate((dk0, dv0, dk1, dv1)):
            if h == 0:
                acc_ref[n] = part
            else:
                acc_ref[n] += part
    at_k = pl.ds(pl.multiple_of(g * HEAD_SIZE, HEAD_SIZE), HEAD_SIZE)
    at_v = pl.ds(
        pl.multiple_of((KEY_VALUE_HEADS + g) * HEAD_SIZE, HEAD_SIZE), HEAD_SIZE
    )
    prev_ref[:, at_k] = (acc_ref[0] * FACTOR).astype(BF16)
    prev_ref[:, at_v] = acc_ref[1].astype(BF16)
    dk_ref[...] = acc_ref[2] * FACTOR
    dv_ref[...] = acc_ref[3]


def local_grads(query, grad, key, value, prev, ext, low):
    wide = pl.BlockSpec((ROWS, GROUP * HEAD_SIZE), lambda g: (0, g))
    narrow = pl.BlockSpec((ROWS, HEAD_SIZE), lambda g: (0, g))
    kv = (ROWS, KEY_VALUE_HEADS * HEAD_SIZE)
    return pl.pallas_call(
        local_kernel,
        grid=(KEY_VALUE_HEADS,),
        in_specs=[
            wide, wide, narrow, narrow, narrow,
            pl.BlockSpec((ROWS, HEAD_SIZE), lambda g: (0, KEY_VALUE_HEADS + g)),
            pl.BlockSpec((ROWS, EXT), lambda g: (0, 0)),
            pl.BlockSpec((8, ROWS), lambda g: (0, 0)),
        ],
        out_specs=[
            wide, narrow, narrow,
            pl.BlockSpec((ROWS, 2 * KEY_VALUE_HEADS * HEAD_SIZE), lambda g: (0, 0)),
        ],
        out_shape=[
            jax.ShapeDtypeStruct((ROWS, QUERY_HEADS * HEAD_SIZE), F32),
            jax.ShapeDtypeStruct(kv, F32),
            jax.ShapeDtypeStruct(kv, F32),
            jax.ShapeDtypeStruct((ROWS, 2 * KEY_VALUE_HEADS * HEAD_SIZE), BF16),
        ],
        scratch_shapes=[
            pltpu.VMEM((EXT, ROWS), F32),
            pltpu.VMEM((4, ROWS, HEAD_SIZE), F32),
        ],
        cost_estimate=pl.CostEstimate(
            flops=16 * 10**9, bytes_accessed=8 << 20, transcendentals=0
        ),
        name="local_grads",
    )(query, grad, key, value, prev, prev, ext, low)


def routed_kernel(half, y_ref, kv_ref, *refs):
    slot_refs, ext_refs, refs = refs[:NX], refs[NX : 2 * NX], refs[2 * NX :]
    dq_refs, dkv_ref = refs[:NX], refs[NX]
    yy = pl.program_id(0)

    @pl.when(yy > y_ref[0])
    def _():
        dkv_ref[...] = jnp.zeros_like(dkv_ref)
        for s in range(NX):
            dq_refs[s][...] = jnp.zeros_like(dq_refs[s])

    @pl.when(yy <= y_ref[0])
    def _():
        ext = jnp.concatenate([r[...].astype(F32) for r in ext_refs], axis=0)
        key = lax.broadcasted_iota(jnp.int32, (ROWS, ROWS), 0).astype(F32)
        for g in range(HEADS_HALF):
            heads = [g * GROUP + h for h in range(GROUP)]
            first = half * HEADS_HALF * GROUP
            stat = jnp.concatenate(
                [pltpu.roll(ext, (EXT - first - j) % EXT, 1) for j in heads], axis=0
            ).T
            lse2 = stat[LSE_AT : LSE_AT + 1, :] * LOG2E
            delta = stat[DELTA_AT : DELTA_AT + 1, :]
            mask = key >= stat[LOW_AT : LOW_AT + 1, :]

            def rows_of(base):
                return jnp.concatenate(
                    [
                        r[:, base + j * HEAD_SIZE : base + (j + 1) * HEAD_SIZE]
                        for j in heads
                        for r in slot_refs
                    ],
                    axis=0,
                )

            queries = rows_of(0)
            grads = rows_of(QW)
            keys = kv_ref[:, g * HEAD_SIZE : (g + 1) * HEAD_SIZE]
            values = kv_ref[:, KW + g * HEAD_SIZE : KW + (g + 1) * HEAD_SIZE]
            dq, dk, dv = tile_grads(keys, values, queries, grads, lse2, delta, mask)
            dkv_ref[:, g * HEAD_SIZE : (g + 1) * HEAD_SIZE] = (dk * FACTOR).astype(BF16)
            dkv_ref[:, KW + g * HEAD_SIZE : KW + (g + 1) * HEAD_SIZE] = dv.astype(BF16)
            dq_low = (dq * FACTOR).astype(BF16)
            for n, j in enumerate(heads):
                for s in range(NX):
                    at = (n * NX + s) * QB
                    dq_refs[s][:, j * HEAD_SIZE : (j + 1) * HEAD_SIZE] = dq_low[at : at + QB]


def routed_grads(half, y, kv_all, slots, ext_slots):
    ext_at = 2 * QW // EXT
    return pl.pallas_call(
        functools.partial(routed_kernel, half),
        grid=(NY,),
        in_specs=[
            pl.BlockSpec(memory_space=pltpu.SMEM),
            pl.BlockSpec((ROWS, 2 * KW), lambda i: (i, 0)),
        ]
        + [pl.BlockSpec((QB, 2 * QW), lambda i: (i, 0))] * NX
        + [pl.BlockSpec((QB, EXT), lambda i: (i, ext_at))] * NX,
        out_specs=[pl.BlockSpec((QB, QW), lambda i: (i, 0))] * NX
        + [pl.BlockSpec((ROWS, 2 * KW), lambda i: (i, 0))],
        out_shape=[jax.ShapeDtypeStruct((SLOTS, QW), BF16)] * NX
        + [jax.ShapeDtypeStruct((NY * ROWS, 2 * KW), BF16)],
        cost_estimate=pl.CostEstimate(
            flops=8 * 10**9, bytes_accessed=8 << 20, transcendentals=0
        ),
        name=f"routed_grads_{half}",
    )(y, kv_all, *slots, *ext_slots)


def join_kernel(inv_ref, dq_ref, *refs):
    out_ref = refs[-1]
    out_ref[...] = dq_ref[...].astype(BF16)

    def one(yy, carry):
        at = pl.ds(pl.multiple_of(yy * QB, QB), QB)
        for s in range(NX):
            found = inv_ref[s * NY + yy]

            @pl.when(found >= 0)
            def _(s=s, found=found):
                rows = pl.ds(pl.multiple_of(found * QB, QB), QB)
                for half in range(HALVES):
                    cols = slice(half * QW, (half + 1) * QW)
                    part = refs[half * NX + s][at, :].astype(F32)
                    out_ref[rows, cols] = (dq_ref[rows, cols] + part).astype(BF16)

        return carry

    lax.fori_loop(0, NY, one, 0)


def join_queries(inv, dq_local, returned):
    vmem = pl.BlockSpec(memory_space=pltpu.VMEM)
    return pl.pallas_call(
        join_kernel,
        in_specs=[pl.BlockSpec(memory_space=pltpu.SMEM), vmem] + [vmem] * (NX * HALVES),
        out_specs=vmem,
        out_shape=jax.ShapeDtypeStruct((ROWS, QUERY_HEADS * HEAD_SIZE), BF16),
        cost_estimate=pl.CostEstimate(
            flops=4 * 10**9, bytes_accessed=6 << 20, transcendentals=0
        ),
        name="join_queries",
    )(inv, dq_local, *returned)


def sum_kernel(dk_ref, dv_ref, back_ref, part_ref, out_k, out_v):
    both = back_ref[...].astype(F32) + part_ref[...].astype(F32)
    out_k[...] = (dk_ref[...] + both[:, :KW]).astype(BF16)
    out_v[...] = (dv_ref[...] + both[:, KW:]).astype(BF16)


def sum_keys(dk, dv, back, part):
    vmem = pl.BlockSpec(memory_space=pltpu.VMEM)
    shape = jax.ShapeDtypeStruct((ROWS, KEY_VALUE_HEADS * HEAD_SIZE), BF16)
    return pl.pallas_call(
        sum_kernel,
        in_specs=[vmem] * 4,
        out_specs=[vmem, vmem],
        out_shape=[shape, shape],
        name="sum_keys",
    )(dk, dv, back, part)


def around(value, steps):
    return lax.ppermute(value, "cp_1", [(i, (i + steps) % NX) for i in range(NX)])


def along(value, steps):
    count = lax.axis_size(GRP_CP)
    first, last = (max(0, -steps), min(count, count - steps))
    return lax.ppermute(value, GRP_CP, [(i, i + steps) for i in range(first, last)])


def on_device(query, key, value, output_gradient, lse, delta, lengths, plan):
    y = lax.axis_index("cp_0")
    x = lax.axis_index("cp_1")
    member = y * NX + x
    shard = lax.axis_index(GRP_CP)
    first_row = shard * ROWS

    kv = jnp.concatenate([key, value], axis=1)
    kv_all = lax.all_gather(kv, "cp_0", axis=0, tiled=True)

    order = jnp.arange(lengths.shape[0], dtype=jnp.int32)
    ends = jnp.sum(jnp.where(order[:, None] <= order[None, :], lengths[:, None], 0), axis=0)
    position = first_row + jnp.arange(ROWS, dtype=jnp.int32)
    doc_start = jnp.max(jnp.where(ends[:, None] <= position[None, :], ends[:, None], 0), axis=0)
    row_plan = jnp.repeat(plan, QB)
    skip_prev = (row_plan == member - 1) & (member >= 1)
    low_local = doc_start - (first_row - ROWS)
    low_local = jnp.where(skip_prev, jnp.maximum(low_local, ROWS), low_local)
    low_local = jnp.broadcast_to(low_local[None, :], (8, ROWS))
    target_row = (shard - member + jnp.maximum(row_plan, 0)) * ROWS
    low_routed = jnp.clip(doc_start - target_row, 0, ROWS).astype(BF16)
    ext = jnp.concatenate(
        [
            lse,
            delta,
            jnp.broadcast_to(low_routed[:, None], (ROWS, QUERY_HEADS)),
            jnp.zeros((ROWS, EXT - 3 * QUERY_HEADS), BF16),
        ],
        axis=1,
    )

    steps = jnp.arange(NX, dtype=jnp.int32)
    targets = jnp.arange(NY, dtype=jnp.int32)[None, :] * NX + ((x + steps) % NX)[:, None]
    hits = plan[None, :] == targets.reshape(-1)[:, None]
    inv = jnp.max(jnp.where(hits, jnp.arange(BLOCKS, dtype=jnp.int32)[None, :], -1), axis=1)

    packed = pack(0, inv, query, output_gradient, ext)
    *packed, kv_shift = lax.optimization_barrier((*packed, kv))
    slots = [packed[0]] + [around(packed[s], s) for s in range(1, NX)]
    prev = along(kv_shift, 1)

    dq_local, dk_own, dv_own, prev_grads = local_grads(
        query, output_gradient, key, value, prev, ext, low_local
    )
    back = along(prev_grads, -1)
    kv_all, dq_local, back = lax.optimization_barrier((kv_all, dq_local, back))

    y_table = jnp.reshape(y, (1,)).astype(jnp.int32)
    *dq_slots, dkv = routed_grads(0, y_table, kv_all, slots, slots)
    part = lax.psum_scatter(dkv, "cp_0", scatter_dimension=0, tiled=True)
    returned = [dq_slots[0]] + [around(dq_slots[s], -s) for s in range(1, NX)]

    dquery = join_queries(inv, dq_local, returned)
    dkey, dvalue = sum_keys(dk_own, dv_own, back, part)
    return dquery, dkey, dvalue


def solution(mesh):
    torus = Mesh(mesh.devices.reshape(mesh.shape["grp"], NY, NX), ("grp", "cp_0", "cp_1"))
    split = P(GRP_CP, None)
    return jax.shard_map(
        on_device,
        mesh=torus,
        in_specs=(split,) * 6 + (P(), P(GRP_CP)),
        out_specs=(split,) * 3,
        check_vma=False,
    )
```

```python
import functools
import math

import jax
import jax.numpy as jnp
from jax import lax
from jax.experimental import pallas as pl
from jax.experimental.pallas import tpu as pltpu
from jax.sharding import Mesh
from jax.sharding import PartitionSpec as P

QUERY_HEADS = 16
KEY_VALUE_HEADS = 4
HEAD_SIZE = 128
GROUP = QUERY_HEADS // KEY_VALUE_HEADS
ROWS = 256
QB = 16
BLOCKS = ROWS // QB
NY = 8
NX = 4
HALVES = 1
PIECES = 2
PIECE_HEADS = KEY_VALUE_HEADS // PIECES
KV = KEY_VALUE_HEADS * HEAD_SIZE
HEADS_HALF = KEY_VALUE_HEADS // HALVES
QW = HEADS_HALF * GROUP * HEAD_SIZE
KW = HEADS_HALF * HEAD_SIZE
SLOTS = NY * QB
EXT = 128
LSE_AT = 0
DELTA_AT = 16
LOW_AT = 32
GRP_CP = ("grp", "cp_0", "cp_1")
FACTOR = HEAD_SIZE ** (-0.5)
LOG2E = math.log2(math.e)

F32 = jnp.float32
BF16 = jnp.bfloat16


def dot_nt(a, b):
    return lax.dot_general(a, b, (((1,), (1,)), ((), ())), preferred_element_type=F32)


def dot_nn(a, b):
    return lax.dot_general(a, b, (((1,), (0,)), ((), ())), preferred_element_type=F32)


def dot_tn(a, b):
    return lax.dot_general(a, b, (((0,), (0,)), ((), ())), preferred_element_type=F32)


def tile_grads(keys, values, queries, grads, lse2, delta, mask):
    scores = dot_nt(keys, queries)
    probs = jnp.where(mask, jnp.exp2(scores * (FACTOR * LOG2E) - lse2), 0.0)
    dprobs = dot_nt(values, grads)
    dscores = probs * (dprobs - delta)
    probs_low = probs.astype(BF16)
    dscores_low = dscores.astype(BF16)
    return (
        dot_tn(dscores_low, keys),
        dot_nn(dscores_low, queries),
        dot_nn(probs_low, grads),
    )


def pack_kernel(with_ext, inv_ref, q_ref, g_ref, ext_ref, *out_refs):
    lane = lax.broadcasted_iota(jnp.int32, (QB, EXT), 1)

    def one(yy, carry):
        to = pl.ds(pl.multiple_of(yy * QB, QB), QB)
        for s in range(NX):
            found = inv_ref[s * NY + yy]
            rows = pl.ds(pl.multiple_of(jnp.maximum(found, 0) * QB, QB), QB)
            out_refs[s][to, 0:QW] = q_ref[rows, :]
            out_refs[s][to, QW : 2 * QW] = g_ref[rows, :]
            if with_ext:
                ext = ext_ref[rows, :].astype(F32)
                low = jnp.where(found >= 0, ext, float(ROWS))
                ext = jnp.where(lane >= LOW_AT, low, ext)
                out_refs[s][to, 2 * QW :] = ext.astype(BF16)
        return carry

    lax.fori_loop(0, NY, one, 0)


def pack(half, inv, query, grad, ext):
    with_ext = half == 0
    width = 2 * QW + (EXT if with_ext else 0)
    spec = pl.BlockSpec((ROWS, QW), lambda i, half=half: (0, half))
    return pl.pallas_call(
        functools.partial(pack_kernel, with_ext),
        grid=(1,),
        in_specs=[
            pl.BlockSpec(memory_space=pltpu.SMEM),
            spec,
            spec,
            pl.BlockSpec((ROWS, EXT), lambda i: (0, 0)),
        ],
        out_specs=[pl.BlockSpec((SLOTS, width), lambda i: (0, 0))] * NX,
        out_shape=[jax.ShapeDtypeStruct((SLOTS, width), BF16)] * NX,
        cost_estimate=pl.CostEstimate(
            flops=4 * 10**9, bytes_accessed=6 << 20, transcendentals=0
        ),
    )(inv, query, grad, ext)


def local_kernel(
    piece, q_ref, g_ref, k_ref, v_ref, pk_ref, pv_ref, ext_ref, low_ref,
    dq_ref, dk_ref, dv_ref, prev_ref, stat_ref, acc_ref,
):
    g = pl.program_id(0)

    @pl.when(g == 0)
    def _():
        stat_ref[...] = ext_ref[...].astype(F32).T

    key = lax.broadcasted_iota(jnp.int32, (ROWS, ROWS), 0)
    row = lax.broadcasted_iota(jnp.int32, (ROWS, ROWS), 1)
    low = low_ref[0:1, :]
    mask_prev = key >= low
    mask_own = (key + ROWS >= low) & (key <= row)
    for h in range(GROUP):
        cols = slice(h * HEAD_SIZE, (h + 1) * HEAD_SIZE)
        queries = q_ref[:, cols]
        grads = g_ref[:, cols]
        head = (piece * PIECE_HEADS + g) * GROUP + h
        lse2 = stat_ref[pl.ds(LSE_AT + head, 1), :] * LOG2E
        delta = stat_ref[pl.ds(DELTA_AT + head, 1), :]
        dq0, dk0, dv0 = tile_grads(
            pk_ref[...], pv_ref[...], queries, grads, lse2, delta, mask_prev
        )
        dq1, dk1, dv1 = tile_grads(
            k_ref[...], v_ref[...], queries, grads, lse2, delta, mask_own
        )
        dq_ref[:, cols] = (dq0 + dq1) * FACTOR
        for n, part in enumerate((dk0, dv0, dk1, dv1)):
            if h == 0:
                acc_ref[n] = part
            else:
                acc_ref[n] += part
    at_k = pl.ds(pl.multiple_of(g * HEAD_SIZE, HEAD_SIZE), HEAD_SIZE)
    at_v = pl.ds(
        pl.multiple_of((PIECE_HEADS + g) * HEAD_SIZE, HEAD_SIZE), HEAD_SIZE
    )
    prev_ref[:, at_k] = (acc_ref[0] * FACTOR).astype(BF16)
    prev_ref[:, at_v] = acc_ref[1].astype(BF16)
    dk_ref[...] = acc_ref[2] * FACTOR
    dv_ref[...] = acc_ref[3]


def local_grads(piece, query, grad, key, value, prev, ext, low):
    first = piece * PIECE_HEADS
    wide = pl.BlockSpec((ROWS, GROUP * HEAD_SIZE), lambda g: (0, first + g))
    narrow = pl.BlockSpec((ROWS, HEAD_SIZE), lambda g: (0, first + g))
    wide_out = pl.BlockSpec((ROWS, GROUP * HEAD_SIZE), lambda g: (0, g))
    narrow_out = pl.BlockSpec((ROWS, HEAD_SIZE), lambda g: (0, g))
    width = PIECE_HEADS * HEAD_SIZE
    return pl.pallas_call(
        functools.partial(local_kernel, piece),
        grid=(PIECE_HEADS,),
        in_specs=[
            wide, wide, narrow, narrow, narrow,
            pl.BlockSpec((ROWS, HEAD_SIZE), lambda g: (0, KEY_VALUE_HEADS + first + g)),
            pl.BlockSpec((ROWS, EXT), lambda g: (0, 0)),
            pl.BlockSpec((8, ROWS), lambda g: (0, 0)),
        ],
        out_specs=[
            wide_out, narrow_out, narrow_out,
            pl.BlockSpec((ROWS, 2 * width), lambda g: (0, 0)),
        ],
        out_shape=[
            jax.ShapeDtypeStruct((ROWS, GROUP * width), F32),
            jax.ShapeDtypeStruct((ROWS, width), F32),
            jax.ShapeDtypeStruct((ROWS, width), F32),
            jax.ShapeDtypeStruct((ROWS, 2 * width), BF16),
        ],
        scratch_shapes=[
            pltpu.VMEM((EXT, ROWS), F32),
            pltpu.VMEM((4, ROWS, HEAD_SIZE), F32),
        ],
        cost_estimate=pl.CostEstimate(
            flops=8 * 10**9, bytes_accessed=4 << 20, transcendentals=0
        ),
    )(query, grad, key, value, prev, prev, ext, low)


def routed_kernel(count, pairs, at_ref, *refs):
    kv_count = 2 if pairs else count
    kv_in, refs = refs[:kv_count], refs[kv_count:]
    slot_refs, ext_refs, refs = refs[:NX], refs[NX : 2 * NX], refs[2 * NX :]
    if not pairs:
        refs = refs[NX:]
    dq_refs, dk_ref, dv_ref, kv_ref = refs[:NX], refs[NX], refs[NX + 1], refs[NX + 2]
    step = pl.program_id(0)
    active = at_ref[step] <= at_ref[count]

    @pl.when(jnp.logical_not(active))
    def _():
        dk_ref[...] = jnp.zeros_like(dk_ref)
        dv_ref[...] = jnp.zeros_like(dv_ref)
        for s in range(NX):
            dq_refs[s][...] = jnp.zeros_like(dq_refs[s])

    if pairs:
        kv_ref[:, :KV] = kv_in[0][...]
        kv_ref[:, KV:] = kv_in[1][...]
    else:
        for n in range(count):

            @pl.when(step == n)
            def _(n=n):
                kv_ref[...] = kv_in[n][...]

    @pl.when(active)
    def _():
        ext = jnp.concatenate([r[...].astype(F32) for r in ext_refs], axis=0)
        key = lax.broadcasted_iota(jnp.int32, (ROWS, ROWS), 0).astype(F32)
        for g in range(HEADS_HALF):
            heads = [g * GROUP + h for h in range(GROUP)]
            stat = jnp.concatenate(
                [pltpu.roll(ext, (EXT - j) % EXT, 1) for j in heads], axis=0
            ).T
            lse2 = stat[LSE_AT : LSE_AT + 1, :] * LOG2E
            delta = stat[DELTA_AT : DELTA_AT + 1, :]
            mask = key >= stat[LOW_AT : LOW_AT + 1, :]

            def rows_of(base):
                return jnp.concatenate(
                    [
                        r[:, base + j * HEAD_SIZE : base + (j + 1) * HEAD_SIZE]
                        for j in heads
                        for r in slot_refs
                    ],
                    axis=0,
                )

            queries = rows_of(0)
            grads = rows_of(QW)
            keys = kv_ref[:, g * HEAD_SIZE : (g + 1) * HEAD_SIZE]
            values = kv_ref[:, KW + g * HEAD_SIZE : KW + (g + 1) * HEAD_SIZE]
            dq, dk, dv = tile_grads(keys, values, queries, grads, lse2, delta, mask)
            dk_ref[:, g * HEAD_SIZE : (g + 1) * HEAD_SIZE] = (dk * FACTOR).astype(BF16)
            dv_ref[:, g * HEAD_SIZE : (g + 1) * HEAD_SIZE] = dv.astype(BF16)
            dq_low = (dq * FACTOR).astype(BF16)
            for n, j in enumerate(heads):
                for s in range(NX):
                    at = (n * NX + s) * QB
                    dq_refs[s][:, j * HEAD_SIZE : (j + 1) * HEAD_SIZE] = dq_low[at : at + QB]


def routed_grads(distances, y, kvs, slots, before=()):
    count = len(distances)
    pairs = not before
    at = (y - jnp.array(distances, jnp.int32)) % NY
    table = jnp.concatenate([at, jnp.reshape(y, (1,))]).astype(jnp.int32)
    ext_at = 2 * QW // EXT
    row = lambda i, t: (t[i], 0)
    whole = [pl.BlockSpec(kv.shape, lambda i, t: (0, 0)) for kv in kvs]
    grads = pl.BlockSpec((None, ROWS, KV), lambda i, t: (i, 0, 0))
    first_before = 1 + len(kvs) + 2 * NX
    return pl.pallas_call(
        functools.partial(routed_kernel, count, pairs),
        grid_spec=pltpu.PrefetchScalarGridSpec(
            num_scalar_prefetch=1,
            grid=(count,),
            in_specs=whole
            + [pl.BlockSpec((QB, 2 * QW), row)] * NX
            + [pl.BlockSpec((QB, EXT), lambda i, t: (t[i], ext_at))] * NX
            + [pl.BlockSpec(memory_space=pl.ANY)] * len(before),
            out_specs=[pl.BlockSpec((QB, QW), row)] * NX + [grads, grads],
            scratch_shapes=[pltpu.VMEM((ROWS, 2 * KV), BF16)],
        ),
        out_shape=[jax.ShapeDtypeStruct((SLOTS, QW), BF16)] * NX
        + [jax.ShapeDtypeStruct((count, ROWS, KV), BF16)] * 2,
        input_output_aliases={first_before + s: s for s in range(len(before))},
        cost_estimate=pl.CostEstimate(
            flops=2 * 10**9 * count, bytes_accessed=1 << 20, transcendentals=0
        ),
    )(table, *kvs, *slots, *slots, *before)


def add_kernel(part_half, dk_ref, dv_ref, got_ref, out_ref):
    for n, part in enumerate((dk_ref, dv_ref)):
        cols = slice(n * KV, (n + 1) * KV)
        if part_half is None:
            got = got_ref[:, cols].astype(F32)
        elif part_half == n:
            got = got_ref[...].astype(F32)
        else:
            out_ref[:, cols] = part[...]
            continue
        out_ref[:, cols] = (part[...].astype(F32) + got).astype(BF16)


def add_grads(n, dk, dv, got, part_half=None):
    spec = pl.BlockSpec((None, ROWS, KV), lambda i: (n, 0, 0))
    return pl.pallas_call(
        functools.partial(add_kernel, part_half),
        grid=(1,),
        in_specs=[spec, spec, pl.BlockSpec(got.shape, lambda i: (0, 0))],
        out_specs=pl.BlockSpec((ROWS, 2 * KV), lambda i: (0, 0)),
        out_shape=jax.ShapeDtypeStruct((ROWS, 2 * KV), BF16),
    )(dk, dv, got)


def join_kernel(inv_ref, *refs):
    dq_refs, refs, out_ref = refs[:PIECES], refs[PIECES:-1], refs[-1]
    wide = QUERY_HEADS * HEAD_SIZE // PIECES
    for p in range(PIECES):
        out_ref[:, p * wide : (p + 1) * wide] = dq_refs[p][...].astype(BF16)

    def one(yy, carry):
        at = pl.ds(pl.multiple_of(yy * QB, QB), QB)
        for s in range(NX):
            found = inv_ref[s * NY + yy]

            @pl.when(found >= 0)
            def _(s=s, found=found):
                rows = pl.ds(pl.multiple_of(found * QB, QB), QB)
                for p in range(PIECES):
                    cols = slice(p * wide, (p + 1) * wide)
                    part = refs[s][at, cols].astype(F32)
                    out_ref[rows, cols] = (dq_refs[p][rows, :] + part).astype(BF16)

        return carry

    lax.fori_loop(0, NY, one, 0)


def join_queries(inv, dq_local, returned):
    vmem = pl.BlockSpec(memory_space=pltpu.VMEM)
    return pl.pallas_call(
        join_kernel,
        in_specs=[pl.BlockSpec(memory_space=pltpu.SMEM)] + [vmem] * (PIECES + NX),
        out_specs=vmem,
        out_shape=jax.ShapeDtypeStruct((ROWS, QUERY_HEADS * HEAD_SIZE), BF16),
        cost_estimate=pl.CostEstimate(
            flops=4 * 10**9, bytes_accessed=6 << 20, transcendentals=0
        ),
        name="join_queries",
    )(inv, *dq_local, *returned)


def sum_kernel(*refs):
    own, back = refs[: 2 * PIECES], refs[2 * PIECES : 3 * PIECES]
    routed, gots, outs = refs[-6:-4], refs[-4:-2], refs[-2:]
    width = KV // PIECES
    for n in range(2):
        for p in range(PIECES):
            cols = slice(p * width, (p + 1) * width)
            far = slice(n * KV + p * width, n * KV + (p + 1) * width)
            total = own[2 * p + n][...] + routed[n][:, cols].astype(F32)
            total += back[p][:, n * width : (n + 1) * width].astype(F32)
            for got in gots:
                total += got[:, far].astype(F32)
            outs[n][:, cols] = total.astype(BF16)


def sum_keys(own, back, at, dk, dv, gots):
    whole = lambda a: pl.BlockSpec(a.shape, lambda i: (0, 0))
    part = pl.BlockSpec((None, ROWS, KV), lambda i: (at, 0, 0))
    shape = jax.ShapeDtypeStruct((ROWS, KV), BF16)
    return pl.pallas_call(
        sum_kernel,
        grid=(1,),
        in_specs=[whole(a) for a in (*own, *back)] + [part, part] + [whole(a) for a in gots],
        out_specs=[pl.BlockSpec((ROWS, KV), lambda i: (0, 0))] * 2,
        out_shape=[shape, shape],
        name="sum_keys",
    )(*own, *back, dk, dv, *gots)


def hop(value, steps):
    return lax.ppermute(value, "cp_0", [(i, (i + steps) % NY) for i in range(NY)])


def beside_kernel(a_ref, b_ref, out_ref):
    out_ref[:, :KV] = a_ref[...]
    out_ref[:, KV:] = b_ref[...]


def beside(a, b):
    vmem = pl.BlockSpec(memory_space=pltpu.VMEM)
    return pl.pallas_call(
        beside_kernel,
        in_specs=[vmem, vmem],
        out_specs=vmem,
        out_shape=jax.ShapeDtypeStruct((ROWS, 2 * KV), BF16),
        name="beside",
    )(a, b)


def around(value, steps):
    return lax.ppermute(value, "cp_1", [(i, (i + steps) % NX) for i in range(NX)])


def along(value, steps):
    count = lax.axis_size(GRP_CP)
    first, last = (max(0, -steps), min(count, count - steps))
    return lax.ppermute(value, GRP_CP, [(i, i + steps) for i in range(first, last)])


def on_device(query, key, value, output_gradient, lse, delta, lengths, plan):
    y = lax.axis_index("cp_0")
    x = lax.axis_index("cp_1")
    member = y * NX + x
    shard = lax.axis_index(GRP_CP)
    first_row = shard * ROWS

    kv = beside(key, value)
    ups, downs = [hop(kv, 1)], [hop(kv, -1)]

    order = jnp.arange(lengths.shape[0], dtype=jnp.int32)
    ends = jnp.sum(jnp.where(order[:, None] <= order[None, :], lengths[:, None], 0), axis=0)
    position = first_row + jnp.arange(ROWS, dtype=jnp.int32)
    doc_start = jnp.max(jnp.where(ends[:, None] <= position[None, :], ends[:, None], 0), axis=0)
    row_plan = jnp.repeat(plan, QB)
    skip_prev = (row_plan == member - 1) & (member >= 1)
    low_local = doc_start - (first_row - ROWS)
    low_local = jnp.where(skip_prev, jnp.maximum(low_local, ROWS), low_local)
    low_local = jnp.broadcast_to(low_local[None, :], (8, ROWS))
    target_row = (shard - member + jnp.maximum(row_plan, 0)) * ROWS
    low_routed = jnp.clip(doc_start - target_row, 0, ROWS).astype(BF16)
    ext = jnp.concatenate(
        [
            lse,
            delta,
            jnp.broadcast_to(low_routed[:, None], (ROWS, QUERY_HEADS)),
            jnp.zeros((ROWS, EXT - 3 * QUERY_HEADS), BF16),
        ],
        axis=1,
    )

    steps = jnp.arange(NX, dtype=jnp.int32)
    targets = jnp.arange(NY, dtype=jnp.int32)[None, :] * NX + ((x + steps) % NX)[:, None]
    hits = plan[None, :] == targets.reshape(-1)[:, None]
    inv = jnp.max(jnp.where(hits, jnp.arange(BLOCKS, dtype=jnp.int32)[None, :], -1), axis=1)

    packed = pack(0, inv, query, output_gradient, ext)
    *packed, kv_shift = lax.optimization_barrier((*packed, kv))
    slots = [packed[0]] + [around(packed[s], s) for s in range(1, NX)]
    prev = along(kv_shift, 1)
    for _ in range(2):
        ups.append(hop(ups[-1], 1))
        downs.append(hop(downs[-1], -1))
    last_up = hop(ups[2][:, :KV], 1)
    last_down = hop(downs[2][:, KV:], -1)

    own, back, dq_local = [], [], []
    held = [(kv, kv)] + list(zip(ups, downs))
    for p in range(PIECES):
        up, down, prev = lax.optimization_barrier((*held[p + 1], prev))
        held[p + 1] = (up, down)
        dq, dk, dv, prev_grads = local_grads(
            p, query, output_gradient, key, value, prev, ext, low_local
        )
        own += [dk, dv]
        dq_local.append(dq)
        back.append(along(prev_grads, -1))
    last_up, last_down, *dq_local = lax.optimization_barrier(
        (last_up, last_down, *dq_local)
    )

    *dq_far, dk_far, dv_far = routed_grads([4], y, [last_up, last_down], slots)
    got_low = hop(dk_far[0], -1)
    got_high = hop(dv_far[0], 1)
    order_near = [3, 5, 2, 6, 1, 7, 0]
    near = [held[3][0], held[3][1], held[2][0], held[2][1], held[1][0], held[1][1], kv]
    *dq_slots, dk_near, dv_near = routed_grads(order_near, y, near, slots, tuple(dq_far))
    returned = [dq_slots[0]] + [around(dq_slots[s], -s) for s in range(1, NX)]
    for n in range(3):
        low = add_grads(2 * n, dk_near, dv_near, got_low, None if n else 0)
        high = add_grads(2 * n + 1, dk_near, dv_near, got_high, None if n else 1)
        got_low = hop(low, -1)
        got_high = hop(high, 1)

    dquery = join_queries(inv, dq_local, returned)
    dkey, dvalue = sum_keys(own, back, 6, dk_near, dv_near, (got_low, got_high))
    return dquery, dkey, dvalue


def solution(mesh):
    torus = Mesh(mesh.devices.reshape(mesh.shape["grp"], NY, NX), ("grp", "cp_0", "cp_1"))
    split = P(GRP_CP, None)

    return jax.shard_map(
        on_device,
        mesh=torus,
        in_specs=(split,) * 6 + (P(), P(GRP_CP)),
        out_specs=(split,) * 3,
        check_vma=False,
    )
```

```python
import functools
import math

import jax
import jax.numpy as jnp
from jax import lax
from jax.experimental import pallas as pl
from jax.experimental.pallas import tpu as pltpu
from jax.sharding import Mesh
from jax.sharding import PartitionSpec as P

QUERY_HEADS = 16
KEY_VALUE_HEADS = 4
HEAD_SIZE = 128
GROUP = QUERY_HEADS // KEY_VALUE_HEADS
ROWS = 256
QB = 16
BLOCKS = ROWS // QB
NY = 8
NX = 4
HALVES = 1
KV = KEY_VALUE_HEADS * HEAD_SIZE
HEADS_HALF = KEY_VALUE_HEADS // HALVES
QW = HEADS_HALF * GROUP * HEAD_SIZE
KW = HEADS_HALF * HEAD_SIZE
SLOTS = NY * QB
EXT = 128
LSE_AT = 0
DELTA_AT = 16
LOW_AT = 32
GRP_CP = ("grp", "cp_0", "cp_1")
FACTOR = HEAD_SIZE ** (-0.5)
LOG2E = math.log2(math.e)

F32 = jnp.float32
BF16 = jnp.bfloat16


def dot_nt(a, b):
    return lax.dot_general(a, b, (((1,), (1,)), ((), ())), preferred_element_type=F32)


def dot_nn(a, b):
    return lax.dot_general(a, b, (((1,), (0,)), ((), ())), preferred_element_type=F32)


def dot_tn(a, b):
    return lax.dot_general(a, b, (((0,), (0,)), ((), ())), preferred_element_type=F32)


def tile_grads(keys, values, queries, grads, lse2, delta, mask):
    scores = dot_nt(keys, queries)
    probs = jnp.where(mask, jnp.exp2(scores * (FACTOR * LOG2E) - lse2), 0.0)
    dprobs = dot_nt(values, grads)
    dscores = probs * (dprobs - delta)
    probs_low = probs.astype(BF16)
    dscores_low = dscores.astype(BF16)
    return (
        dot_tn(dscores_low, keys),
        dot_nn(dscores_low, queries),
        dot_nn(probs_low, grads),
    )


def pack_kernel(with_ext, inv_ref, q_ref, g_ref, ext_ref, *out_refs):
    lane = lax.broadcasted_iota(jnp.int32, (QB, EXT), 1)

    def one(yy, carry):
        to = pl.ds(pl.multiple_of(yy * QB, QB), QB)
        for s in range(NX):
            found = inv_ref[s * NY + yy]
            rows = pl.ds(pl.multiple_of(jnp.maximum(found, 0) * QB, QB), QB)
            out_refs[s][to, 0:QW] = q_ref[rows, :]
            out_refs[s][to, QW : 2 * QW] = g_ref[rows, :]
            if with_ext:
                ext = ext_ref[rows, :].astype(F32)
                low = jnp.where(found >= 0, ext, float(ROWS))
                ext = jnp.where(lane >= LOW_AT, low, ext)
                out_refs[s][to, 2 * QW :] = ext.astype(BF16)
        return carry

    lax.fori_loop(0, NY, one, 0)


def pack(half, inv, query, grad, ext):
    with_ext = half == 0
    width = 2 * QW + (EXT if with_ext else 0)
    spec = pl.BlockSpec((ROWS, QW), lambda i, half=half: (0, half))
    return pl.pallas_call(
        functools.partial(pack_kernel, with_ext),
        grid=(1,),
        in_specs=[
            pl.BlockSpec(memory_space=pltpu.SMEM),
            spec,
            spec,
            pl.BlockSpec((ROWS, EXT), lambda i: (0, 0)),
        ],
        out_specs=[pl.BlockSpec((SLOTS, width), lambda i: (0, 0))] * NX,
        out_shape=[jax.ShapeDtypeStruct((SLOTS, width), BF16)] * NX,
        cost_estimate=pl.CostEstimate(
            flops=4 * 10**9, bytes_accessed=6 << 20, transcendentals=0
        ),
    )(inv, query, grad, ext)


def local_kernel(
    q_ref, g_ref, k_ref, v_ref, pk_ref, pv_ref, ext_ref, low_ref,
    dq_ref, dk_ref, dv_ref, prev_ref, stat_ref, acc_ref,
):
    g = pl.program_id(0)

    @pl.when(g == 0)
    def _():
        stat_ref[...] = ext_ref[...].astype(F32).T

    key = lax.broadcasted_iota(jnp.int32, (ROWS, ROWS), 0)
    row = lax.broadcasted_iota(jnp.int32, (ROWS, ROWS), 1)
    low = low_ref[0:1, :]
    mask_prev = key >= low
    mask_own = (key + ROWS >= low) & (key <= row)
    for h in range(GROUP):
        cols = slice(h * HEAD_SIZE, (h + 1) * HEAD_SIZE)
        queries = q_ref[:, cols]
        grads = g_ref[:, cols]
        head = g * GROUP + h
        lse2 = stat_ref[pl.ds(LSE_AT + head, 1), :] * LOG2E
        delta = stat_ref[pl.ds(DELTA_AT + head, 1), :]
        dq0, dk0, dv0 = tile_grads(
            pk_ref[...], pv_ref[...], queries, grads, lse2, delta, mask_prev
        )
        dq1, dk1, dv1 = tile_grads(
            k_ref[...], v_ref[...], queries, grads, lse2, delta, mask_own
        )
        dq_ref[:, cols] = (dq0 + dq1) * FACTOR
        for n, part in enumerate((dk0, dv0, dk1, dv1)):
            if h == 0:
                acc_ref[n] = part
            else:
                acc_ref[n] += part
    at_k = pl.ds(pl.multiple_of(g * HEAD_SIZE, HEAD_SIZE), HEAD_SIZE)
    at_v = pl.ds(
        pl.multiple_of((KEY_VALUE_HEADS + g) * HEAD_SIZE, HEAD_SIZE), HEAD_SIZE
    )
    prev_ref[:, at_k] = (acc_ref[0] * FACTOR).astype(BF16)
    prev_ref[:, at_v] = acc_ref[1].astype(BF16)
    dk_ref[...] = acc_ref[2] * FACTOR
    dv_ref[...] = acc_ref[3]


def local_grads(query, grad, key, value, prev, ext, low):
    wide = pl.BlockSpec((ROWS, GROUP * HEAD_SIZE), lambda g: (0, g))
    narrow = pl.BlockSpec((ROWS, HEAD_SIZE), lambda g: (0, g))
    kv = (ROWS, KEY_VALUE_HEADS * HEAD_SIZE)
    return pl.pallas_call(
        local_kernel,
        grid=(KEY_VALUE_HEADS,),
        in_specs=[
            wide, wide, narrow, narrow, narrow,
            pl.BlockSpec((ROWS, HEAD_SIZE), lambda g: (0, KEY_VALUE_HEADS + g)),
            pl.BlockSpec((ROWS, EXT), lambda g: (0, 0)),
            pl.BlockSpec((8, ROWS), lambda g: (0, 0)),
        ],
        out_specs=[
            wide, narrow, narrow,
            pl.BlockSpec((ROWS, 2 * KEY_VALUE_HEADS * HEAD_SIZE), lambda g: (0, 0)),
        ],
        out_shape=[
            jax.ShapeDtypeStruct((ROWS, QUERY_HEADS * HEAD_SIZE), F32),
            jax.ShapeDtypeStruct(kv, F32),
            jax.ShapeDtypeStruct(kv, F32),
            jax.ShapeDtypeStruct((ROWS, 2 * KEY_VALUE_HEADS * HEAD_SIZE), BF16),
        ],
        scratch_shapes=[
            pltpu.VMEM((EXT, ROWS), F32),
            pltpu.VMEM((4, ROWS, HEAD_SIZE), F32),
        ],
        cost_estimate=pl.CostEstimate(
            flops=16 * 10**9, bytes_accessed=8 << 20, transcendentals=0
        ),
        name="local_grads",
    )(query, grad, key, value, prev, prev, ext, low)


def routed_kernel(half, y_ref, kv_ref, *refs):
    slot_refs, ext_refs, refs = refs[:NX], refs[NX : 2 * NX], refs[2 * NX :]
    dq_refs, dkv_ref = refs[:NX], refs[NX]
    yy = pl.program_id(0)

    @pl.when(yy > y_ref[0])
    def _():
        dkv_ref[...] = jnp.zeros_like(dkv_ref)
        for s in range(NX):
            dq_refs[s][...] = jnp.zeros_like(dq_refs[s])

    @pl.when(yy <= y_ref[0])
    def _():
        ext = jnp.concatenate([r[...].astype(F32) for r in ext_refs], axis=0)
        key = lax.broadcasted_iota(jnp.int32, (ROWS, ROWS), 0).astype(F32)
        for g in range(HEADS_HALF):
            heads = [g * GROUP + h for h in range(GROUP)]
            first = half * HEADS_HALF * GROUP
            stat = jnp.concatenate(
                [pltpu.roll(ext, (EXT - first - j) % EXT, 1) for j in heads], axis=0
            ).T
            lse2 = stat[LSE_AT : LSE_AT + 1, :] * LOG2E
            delta = stat[DELTA_AT : DELTA_AT + 1, :]
            mask = key >= stat[LOW_AT : LOW_AT + 1, :]

            def rows_of(base):
                return jnp.concatenate(
                    [
                        r[:, base + j * HEAD_SIZE : base + (j + 1) * HEAD_SIZE]
                        for j in heads
                        for r in slot_refs
                    ],
                    axis=0,
                )

            queries = rows_of(0)
            grads = rows_of(QW)
            keys = kv_ref[:, g * HEAD_SIZE : (g + 1) * HEAD_SIZE]
            values = kv_ref[:, KW + g * HEAD_SIZE : KW + (g + 1) * HEAD_SIZE]
            dq, dk, dv = tile_grads(keys, values, queries, grads, lse2, delta, mask)
            dkv_ref[:, g * HEAD_SIZE : (g + 1) * HEAD_SIZE] = (dk * FACTOR).astype(BF16)
            dkv_ref[:, KW + g * HEAD_SIZE : KW + (g + 1) * HEAD_SIZE] = dv.astype(BF16)
            dq_low = (dq * FACTOR).astype(BF16)
            for n, j in enumerate(heads):
                for s in range(NX):
                    at = (n * NX + s) * QB
                    dq_refs[s][:, j * HEAD_SIZE : (j + 1) * HEAD_SIZE] = dq_low[at : at + QB]


def routed_grads(half, y, kv_all, slots, ext_slots):
    ext_at = 2 * QW // EXT
    return pl.pallas_call(
        functools.partial(routed_kernel, half),
        grid=(NY,),
        in_specs=[
            pl.BlockSpec(memory_space=pltpu.SMEM),
            pl.BlockSpec((ROWS, 2 * KW), lambda i: (i, 0)),
        ]
        + [pl.BlockSpec((QB, 2 * QW), lambda i: (i, 0))] * NX
        + [pl.BlockSpec((QB, EXT), lambda i: (i, ext_at))] * NX,
        out_specs=[pl.BlockSpec((QB, QW), lambda i: (i, 0))] * NX
        + [pl.BlockSpec((ROWS, 2 * KW), lambda i: (i, 0))],
        out_shape=[jax.ShapeDtypeStruct((SLOTS, QW), BF16)] * NX
        + [jax.ShapeDtypeStruct((NY * ROWS, 2 * KW), BF16)],
        cost_estimate=pl.CostEstimate(
            flops=8 * 10**9, bytes_accessed=8 << 20, transcendentals=0
        ),
    )(y, kv_all, *slots, *ext_slots)


def join_kernel(inv_ref, dq_ref, *refs):
    out_ref = refs[-1]
    out_ref[...] = dq_ref[...].astype(BF16)

    def one(yy, carry):
        at = pl.ds(pl.multiple_of(yy * QB, QB), QB)
        for s in range(NX):
            found = inv_ref[s * NY + yy]

            @pl.when(found >= 0)
            def _(s=s, found=found):
                rows = pl.ds(pl.multiple_of(found * QB, QB), QB)
                for half in range(HALVES):
                    cols = slice(half * QW, (half + 1) * QW)
                    part = refs[half * NX + s][at, :].astype(F32)
                    out_ref[rows, cols] = (dq_ref[rows, cols] + part).astype(BF16)

        return carry

    lax.fori_loop(0, NY, one, 0)


def join_queries(inv, dq_local, returned):
    vmem = pl.BlockSpec(memory_space=pltpu.VMEM)
    return pl.pallas_call(
        join_kernel,
        in_specs=[pl.BlockSpec(memory_space=pltpu.SMEM), vmem] + [vmem] * (NX * HALVES),
        out_specs=vmem,
        out_shape=jax.ShapeDtypeStruct((ROWS, QUERY_HEADS * HEAD_SIZE), BF16),
        cost_estimate=pl.CostEstimate(
            flops=4 * 10**9, bytes_accessed=6 << 20, transcendentals=0
        ),
        name="join_queries",
    )(inv, dq_local, *returned)


def sum_kernel(dk_ref, dv_ref, back_ref, part_ref, out_k, out_v):
    both = back_ref[...].astype(F32) + part_ref[...].astype(F32)
    out_k[...] = (dk_ref[...] + both[:, :KW]).astype(BF16)
    out_v[...] = (dv_ref[...] + both[:, KW:]).astype(BF16)


def sum_keys(dk, dv, back, part):
    vmem = pl.BlockSpec(memory_space=pltpu.VMEM)
    shape = jax.ShapeDtypeStruct((ROWS, KEY_VALUE_HEADS * HEAD_SIZE), BF16)
    return pl.pallas_call(
        sum_kernel,
        in_specs=[vmem] * 4,
        out_specs=[vmem, vmem],
        out_shape=[shape, shape],
        name="sum_keys",
    )(dk, dv, back, part)


def beside_kernel(a_ref, b_ref, out_ref):
    out_ref[:, :KV] = a_ref[...]
    out_ref[:, KV:] = b_ref[...]


def beside(a, b):
    vmem = pl.BlockSpec(memory_space=pltpu.VMEM)
    return pl.pallas_call(
        beside_kernel,
        in_specs=[vmem, vmem],
        out_specs=vmem,
        out_shape=jax.ShapeDtypeStruct((ROWS, 2 * KV), BF16),
        name="beside",
    )(a, b)


def around(value, steps):
    return lax.ppermute(value, "cp_1", [(i, (i + steps) % NX) for i in range(NX)])


def along(value, steps):
    count = lax.axis_size(GRP_CP)
    first, last = (max(0, -steps), min(count, count - steps))
    return lax.ppermute(value, GRP_CP, [(i, i + steps) for i in range(first, last)])


def on_device(query, key, value, output_gradient, lse, delta, lengths, plan):
    y = lax.axis_index("cp_0")
    x = lax.axis_index("cp_1")
    member = y * NX + x
    shard = lax.axis_index(GRP_CP)
    first_row = shard * ROWS

    kv = beside(key, value)
    kv_all = lax.all_gather(kv, "cp_0", axis=0, tiled=True)

    order = jnp.arange(lengths.shape[0], dtype=jnp.int32)
    ends = jnp.sum(jnp.where(order[:, None] <= order[None, :], lengths[:, None], 0), axis=0)
    position = first_row + jnp.arange(ROWS, dtype=jnp.int32)
    doc_start = jnp.max(jnp.where(ends[:, None] <= position[None, :], ends[:, None], 0), axis=0)
    row_plan = jnp.repeat(plan, QB)
    skip_prev = (row_plan == member - 1) & (member >= 1)
    low_local = doc_start - (first_row - ROWS)
    low_local = jnp.where(skip_prev, jnp.maximum(low_local, ROWS), low_local)
    low_local = jnp.broadcast_to(low_local[None, :], (8, ROWS))
    target_row = (shard - member + jnp.maximum(row_plan, 0)) * ROWS
    low_routed = jnp.clip(doc_start - target_row, 0, ROWS).astype(BF16)
    ext = jnp.concatenate(
        [
            lse,
            delta,
            jnp.broadcast_to(low_routed[:, None], (ROWS, QUERY_HEADS)),
            jnp.zeros((ROWS, EXT - 3 * QUERY_HEADS), BF16),
        ],
        axis=1,
    )

    steps = jnp.arange(NX, dtype=jnp.int32)
    targets = jnp.arange(NY, dtype=jnp.int32)[None, :] * NX + ((x + steps) % NX)[:, None]
    hits = plan[None, :] == targets.reshape(-1)[:, None]
    inv = jnp.max(jnp.where(hits, jnp.arange(BLOCKS, dtype=jnp.int32)[None, :], -1), axis=1)

    prev = along(kv, 1)
    packed = pack(0, inv, query, output_gradient, ext)
    slots = [packed[0]] + [around(packed[s], s) for s in range(1, NX)]

    dq_local, dk_own, dv_own, prev_grads = local_grads(
        query, output_gradient, key, value, prev, ext, low_local
    )
    kv_all, dq_local, prev_grads = lax.optimization_barrier(
        (kv_all, dq_local, prev_grads)
    )
    back = along(prev_grads, -1)

    y_table = jnp.reshape(y, (1,)).astype(jnp.int32)
    *dq_slots, dkv = routed_grads(0, y_table, kv_all, slots, slots)
    part = lax.psum_scatter(dkv, "cp_0", scatter_dimension=0, tiled=True)
    returned = [dq_slots[0]] + [around(dq_slots[s], -s) for s in range(1, NX)]

    dquery = join_queries(inv, dq_local, returned)
    dkey, dvalue = sum_keys(dk_own, dv_own, back, part)
    return dquery, dkey, dvalue


def solution(mesh):
    torus = Mesh(mesh.devices.reshape(mesh.shape["grp"], NY, NX), ("grp", "cp_0", "cp_1"))
    split = P(GRP_CP, None)

    return jax.shard_map(
        on_device,
        mesh=torus,
        in_specs=(split,) * 6 + (P(), P(GRP_CP)),
        out_specs=(split,) * 3,
        check_vma=False,
    )
```
